8 devices in a mesh: b: 1 (over z), rep: 2 (over y), col: 2 (over x), row: 2 (over core).
Axes of the slice: x: 2, y: 2, z: 1, core: 2. Of those that a mesh axis runs over, the one named last changes fastest.
Arguments:
- a_blocks: float32 [28, 28, 128, 128], P(('b', 'row'), 'col')
Outputs:
- output: float32 [28, 28, 128, 128], P(('b', 'row'), 'col')
All inputs are finite; a program needn't handle non-finite values.
Results may differ from the reference program's by a relative error of at most 0.001.
Values sent between devices are 32-bit elements.
A program may use at most 1 GiB of HBM per device.

```python
import jax
import jax.numpy as jnp
from jax import lax

N = 3584
NB = 128
ROW = 2
COL = 2
RANK = N // 8
NUM_BLK = N // NB
ROW_BLK = NUM_BLK // ROW
COL_BLK = NUM_BLK // COL


def to_cyclic(natural):
    grid_view = natural.reshape(ROW_BLK, ROW, NB, COL_BLK, COL, NB)
    return grid_view.transpose(1, 0, 4, 3, 2, 5).reshape(NUM_BLK, NUM_BLK, NB, NB)


def from_cyclic(blocks):
    grid_view = blocks.reshape(ROW, ROW_BLK, COL, COL_BLK, NB, NB)
    return grid_view.transpose(1, 0, 4, 3, 2, 5).reshape(N, N)


def setup_inputs(seed: int = 0, part: int = 0) -> dict:
    base_key = jax.random.fold_in(jax.random.key(seed), part)
    factor = jax.random.normal(base_key, (N, RANK), jnp.float32)
    gram_mat = jnp.dot(factor, factor.T, precision=lax.Precision.HIGHEST, preferred_element_type=jnp.float32)
    spd_mat = 0.5 * (gram_mat + gram_mat.T) + RANK * jnp.eye(N, dtype=jnp.float32)
    return {"a_blocks": to_cyclic(spd_mat)}


def reference(a_blocks):
    lower_fac = jnp.tril(jnp.linalg.cholesky(from_cyclic(a_blocks)))
    return to_cyclic(lower_fac)
```

```python
import functools

import jax
import jax.numpy as jnp
from jax import lax
from jax.experimental import pallas as pl
from jax.experimental.pallas import tpu as pltpu
from jax.sharding import PartitionSpec as P

NB = 128
SUB = 8
F32 = jnp.float32
BF16 = jnp.bfloat16


def split3(x):
    hi = x.astype(BF16)
    rest = x - hi.astype(F32)
    mid = rest.astype(BF16)
    low = (rest - mid.astype(F32)).astype(BF16)
    return hi, mid, low


def dot_nt(a, b):
    return lax.dot_general(a, b, (((1,), (1,)), ((), ())), preferred_element_type=F32)


def dot_nn(a, b):
    return lax.dot_general(a, b, (((1,), (0,)), ((), ())), preferred_element_type=F32)


def six(dot, a, b):
    ah, am, al = a
    bh, bm, bl = b
    small = dot(al, bh) + dot(ah, bl) + dot(am, bm)
    return (small + (dot(am, bh) + dot(ah, bm))) + dot(ah, bh)


def factor_rows(cols, rows):
    sub = lax.broadcasted_iota(jnp.int32, (SUB, NB), 0)
    for k in range(SUB):
        inv_root = lax.rsqrt(jnp.broadcast_to(cols[k][k:k + 1, :], (SUB, NB)))
        scaled = cols[k] * inv_root
        mult = jnp.where(sub > k, scaled, 0.0)
        for c in range(k + 1, SUB):
            cols[c] = cols[c] - scaled * jnp.broadcast_to(scaled[c:c + 1, :], (SUB, NB))
        new_rows = []
        for row in rows:
            pivot_row = jnp.broadcast_to(row[k:k + 1, :], (SUB, NB)) * inv_root
            new_rows.append(jnp.where(sub == k, pivot_row, row - mult * pivot_row))
        rows = new_rows
    return rows


def factor_block(slabs):
    steps = NB // SUB
    sub = lax.broadcasted_iota(jnp.int32, (SUB, NB), 0)
    lane = lax.broadcasted_iota(jnp.int32, (SUB, NB), 1)
    rows = [[slabs[t], jnp.where(lane == sub + SUB * t, 1.0, 0.0).astype(F32)] for t in range(steps)]
    cols = [jnp.broadcast_to(rows[0][0][:, c:c + 1], (SUB, NB)) for c in range(SUB)]
    for t in range(steps):
        rows[t] = factor_rows(cols, rows[t])
        for s in range(t + 1, steps):
            index = sub + SUB * s
            fac, inv = rows[s]
            if s == t + 1:
                cols = [jnp.broadcast_to(fac[:, SUB * s + c:SUB * s + c + 1], (SUB, NB)) for c in range(SUB)]
            for k in range(SUB):
                fac_row = jnp.broadcast_to(rows[t][0][k:k + 1, :], (SUB, NB))
                inv_row = jnp.broadcast_to(rows[t][1][k:k + 1, :], (SUB, NB))
                col = jnp.take_along_axis(fac_row, index, axis=1)
                fac = fac - col * fac_row
                inv = inv - col * inv_row
                if s == t + 1:
                    for c in range(SUB):
                        cols[c] = cols[c] - col * jnp.broadcast_to(col[c:c + 1, :], (SUB, NB))
            rows[s] = [fac, inv]
    upper = [jnp.where(lane >= sub + SUB * t, rows[t][0], 0.0) for t in range(steps)]
    inverse = [jnp.where(lane <= sub + SUB * t, rows[t][1], 0.0) for t in range(steps)]
    return upper, inverse


def kernel(n, src, out, tiles, hi, mid, low, invs, upper, blk_inv, zero, in_sem, out_sem, zero_sem):
    W = 2 * NB
    my_row = lax.axis_index("row")
    my_col = lax.axis_index("col")

    def col_start(p):
        return p * n - (p * (p - 1)) // 2

    def tile_row(big, p):
        return pl.multiple_of((col_start(p) + big - p) * W, W)

    def load_tile(p, big):
        row = tile_row(big, p)
        for r in range(2):
            for c in range(2):
                pltpu.make_async_copy(
                    src.at[r, c, big, p],
                    tiles.at[pl.ds(row + r * NB, NB), pl.ds(c * NB, NB)],
                    in_sem.at[p],
                ).start()

    zero[...] = jnp.zeros_like(zero)

    @pl.loop(0, n)
    def _(p):
        @pl.loop(p, n)
        def _(big):
            load_tile(p, big)

    @pl.loop(0, n)
    def _(p):
        @pl.loop(0, p)
        def _(big):
            pltpu.make_async_copy(zero, out.at[big, p], zero_sem).start()

    @pl.loop(0, n)
    def _(p):
        @pl.loop(p, n)
        def _(big):
            ref = tiles.at[pl.ds(tile_row(big, p), W), :]
            pltpu.make_async_copy(ref, ref, in_sem.at[p]).wait()

    def factor(row, off, which):
        up, inv = factor_block([tiles[pl.ds(row + off + SUB * t, SUB), pl.ds(off, NB)] for t in range(NB // SUB)])
        for t in range(NB // SUB):
            upper[SUB * t:SUB * (t + 1), :] = up[t]
            blk_inv[which, SUB * t:SUB * (t + 1), :] = inv[t]
        tiles[pl.ds(row + off, NB), pl.ds(off, NB)] = upper[...].T

    @pl.loop(0, n)
    def _(s):
        row = tile_row(s, s)
        factor(row, 0, 0)
        inv1 = split3(blk_inv[0])
        l21 = six(dot_nt, split3(tiles[pl.ds(row + NB, NB), 0:NB]), inv1)
        tiles[pl.ds(row + NB, NB), 0:NB] = l21
        l21_parts = split3(l21)
        tiles[pl.ds(row + NB, NB), NB:W] = tiles[pl.ds(row + NB, NB), NB:W] - six(dot_nt, l21_parts, l21_parts)
        factor(row, NB, 1)
        tiles[pl.ds(row, NB), NB:W] = jnp.zeros((NB, NB), F32)
        inv2 = split3(blk_inv[1])
        cross = six(dot_nn, split3(six(dot_nn, inv2, l21_parts)), inv1)
        for part in range(3):
            invs[part, 0:NB, 0:NB] = inv1[part]
            invs[part, NB:W, NB:W] = inv2[part]
            invs[part, 0:NB, NB:W] = jnp.zeros((NB, NB), BF16)
        for part, val in enumerate(split3(-cross)):
            invs[part, NB:W, 0:NB] = val

        @pl.loop(s + 1, n)
        def _(big):
            trow = tile_row(big, s)
            a = split3(tiles[pl.ds(trow, W), :])
            sol = six(dot_nt, a, (invs[0], invs[1], invs[2]))
            tiles[pl.ds(trow, W), :] = sol
            h, m, l = split3(sol)
            prow = pl.multiple_of(big * W, W)
            hi[pl.ds(prow, W), :] = h
            mid[pl.ds(prow, W), :] = m
            low[pl.ds(prow, W), :] = l

        @pl.loop(s, n)
        def _(big):
            pltpu.make_async_copy(
                tiles.at[pl.ds(tile_row(big, s) + pl.multiple_of(my_row * NB, NB), NB), pl.ds(pl.multiple_of(my_col * NB, NB), NB)],
                out.at[big, s],
                out_sem,
            ).start()

        @pl.loop(s + 1, n)
        def _(p):
            prow = pl.multiple_of(p * W, W)
            @pl.loop(p, n)
            def _(big):
                brow = pl.multiple_of(big * W, W)
                a = tuple(ref[pl.ds(brow, W), :] for ref in (hi, mid, low))
                b = tuple(ref[pl.ds(prow, W), :] for ref in (hi, mid, low))
                trow = tile_row(big, p)
                tiles[pl.ds(trow, W), :] = tiles[pl.ds(trow, W), :] - six(dot_nt, a, b)

    @pl.loop(0, n)
    def _(p):
        @pl.loop(p, n)
        def _(big):
            pltpu.make_async_copy(
                tiles.at[pl.ds(tile_row(big, p) + pl.multiple_of(my_row * NB, NB), NB), pl.ds(pl.multiple_of(my_col * NB, NB), NB)],
                out.at[big, p],
                out_sem,
            ).wait()

    @pl.loop(0, n)
    def _(p):
        @pl.loop(0, p)
        def _(big):
            pltpu.make_async_copy(zero, out.at[big, p], zero_sem).wait()


def solution(mesh):
    grid_spec = P(("b", "row"), "col")

    def local_factor(a_loc):
        n = a_loc.shape[0]
        W = 2 * NB
        gathered = lax.all_gather(lax.all_gather(a_loc, "col"), "row")
        return pl.pallas_call(
            functools.partial(kernel, n),
            out_shape=jax.ShapeDtypeStruct(a_loc.shape, F32),
            in_specs=[pl.BlockSpec(memory_space=pl.ANY)],
            out_specs=pl.BlockSpec(memory_space=pl.ANY),
            scratch_shapes=[
                pltpu.VMEM((n * (n + 1) // 2 * W, W), F32),
                pltpu.VMEM((n * W, W), BF16),
                pltpu.VMEM((n * W, W), BF16),
                pltpu.VMEM((n * W, W), BF16),
                pltpu.VMEM((3, W, W), BF16),
                pltpu.VMEM((NB, NB), F32),
                pltpu.VMEM((2, NB, NB), F32),
                pltpu.VMEM((NB, NB), F32),
                pltpu.SemaphoreType.DMA((n,)),
                pltpu.SemaphoreType.DMA,
                pltpu.SemaphoreType.DMA,
            ],
            compiler_params=pltpu.CompilerParams(vmem_limit_bytes=60 << 20),
        )(gathered)

    return jax.shard_map(local_factor, mesh=mesh, in_specs=grid_spec, out_specs=grid_spec, check_vma=False)
```

```python
import functools

import jax
import jax.numpy as jnp
from jax import lax
from jax.experimental import pallas as pl
from jax.experimental.pallas import tpu as pltpu
from jax.sharding import PartitionSpec as P

NB = 128
SUB = 8
F32 = jnp.float32
BF16 = jnp.bfloat16


def split3(x):
    hi = x.astype(BF16)
    rest = x - hi.astype(F32)
    mid = rest.astype(BF16)
    low = (rest - mid.astype(F32)).astype(BF16)
    return hi, mid, low


def dot_nt(a, b):
    return lax.dot_general(a, b, (((1,), (1,)), ((), ())), preferred_element_type=F32)


def dot_nn(a, b):
    return lax.dot_general(a, b, (((1,), (0,)), ((), ())), preferred_element_type=F32)


def six(dot, a, b):
    ah, am, al = a
    bh, bm, bl = b
    small = dot(al, bh) + dot(ah, bl) + dot(am, bm)
    return (small + (dot(am, bh) + dot(ah, bm))) + dot(ah, bh)


def spread_row(x, k):
    return jnp.broadcast_to(x[k:k + 1, :], (SUB, NB))


def spread_cols(x, first):
    return [jnp.broadcast_to(x[:, first + c:first + c + 1], (SUB, NB)) for c in range(SUB)]


def factor_block(load, store):
    steps = NB // SUB
    sub = lax.broadcasted_iota(jnp.int32, (SUB, NB), 0)
    lane = lax.broadcasted_iota(jnp.int32, (SUB, NB), 1)
    rows = [[load(t), jnp.where(lane == sub + SUB * t, 1.0, 0.0).astype(F32)] for t in range(steps)]
    main = spread_cols(rows[0][0], 0)
    ext = spread_cols(rows[1][0], 0)
    for t in range(steps):
        fac, inv = rows[t]
        fac_rows, inv_rows, below = [], [], []
        for k in range(SUB):
            inv_root = lax.rsqrt(spread_row(main[k], k))
            scaled = main[k] * inv_root
            scaled_ext = ext[k] * inv_root if t + 1 < steps else None
            below.append(scaled_ext)
            for c in range(k + 1, SUB):
                factor_c = spread_row(scaled, c)
                main[c] = main[c] - scaled * factor_c
                if t + 1 < steps:
                    ext[c] = ext[c] - scaled_ext * factor_c
            mult = jnp.where(sub > k, scaled, 0.0)
            fac_row = spread_row(fac, k) * inv_root
            inv_row = spread_row(inv, k) * inv_root
            fac = jnp.where(sub == k, fac_row, fac - mult * fac_row)
            inv = jnp.where(sub == k, inv_row, inv - mult * inv_row)
            fac_rows.append(fac_row)
            inv_rows.append(inv_row)
        store(t, jnp.where(lane >= sub + SUB * t, fac, 0.0), jnp.where(lane <= sub + SUB * t, inv, 0.0))
        if t + 1 == steps:
            break
        s = t + 1
        next_main = spread_cols(rows[s][0], SUB * s)
        for k in range(SUB):
            rows[s][0] = rows[s][0] - below[k] * fac_rows[k]
            rows[s][1] = rows[s][1] - below[k] * inv_rows[k]
            for c in range(SUB):
                next_main[c] = next_main[c] - below[k] * spread_row(below[k], c)
        if s + 1 < steps:
            turned = fac.T
            next_ext = spread_cols(rows[s + 1][0], SUB * s)
            for q in range(t + 2, steps):
                for k in range(SUB):
                    col = jnp.broadcast_to(turned[SUB * q:SUB * (q + 1), k:k + 1], (SUB, NB))
                    rows[q][0] = rows[q][0] - col * fac_rows[k]
                    rows[q][1] = rows[q][1] - col * inv_rows[k]
                    if q == t + 2:
                        for c in range(SUB):
                            next_ext[c] = next_ext[c] - col * spread_row(below[k], c)
            ext = next_ext
        main = next_main


def kernel(n, src, out, tiles, hi, mid, low, invs, upper, blk, blk_inv, zero,
           loc_sem, sib_sem, nbr_sem, panel_sem, diag_sem, diag_send_sem, block_send_sem, panel_send_sem,
           out_sem, zero_sem):
    W = 2 * NB
    my_row = lax.axis_index("row")
    my_col = lax.axis_index("col")
    sibling = {"row": 1 - my_row}
    aligned = my_row == my_col
    num_own = n // 2

    barrier = pltpu.get_barrier_semaphore()
    pl.semaphore_signal(barrier, inc=1, device_id=sibling, device_id_type=pl.DeviceIdType.MESH)
    for core in range(2):
        pl.semaphore_signal(barrier, inc=1, device_id={"col": 1 - my_col, "row": core},
                            device_id_type=pl.DeviceIdType.MESH)
    pl.semaphore_wait(barrier, 3)

    def tile_row(big, p):
        return pl.multiple_of((p * n - (p * (p - 1)) // 2 + big - p) * W, W)

    def quadrant(big, p, r, c):
        return tiles.at[pl.ds(pl.multiple_of(tile_row(big, p) + r * NB, NB), NB), pl.ds(pl.multiple_of(c * NB, NB), NB)]

    def tile_ref(big, p):
        return tiles.at[pl.ds(tile_row(big, p), W), :]

    def first_own(p):
        return p + lax.rem(p + my_row, 2)

    def first_other(p):
        return p + lax.rem(p + 1 + my_row, 2)

    def own_tiles(p):
        first = first_own(p)
        return first, lax.div(n + 1 - first, 2)

    def other_tiles(p):
        first = first_other(p)
        return first, lax.div(n + 1 - first, 2)

    def own_loop(p, fn):
        first, count = own_tiles(p)

        @pl.loop(0, count)
        def _(q):
            fn(first + 2 * q)

    def other_loop(p, fn):
        first, count = other_tiles(p)

        @pl.loop(0, count)
        def _(q):
            fn(first + 2 * q)

    def local_copy(block, dst, big, p):
        return pltpu.make_async_copy(block, dst, loc_sem.at[p, lax.div(big, 2)])

    def remote(block, dst, recv, send, device):
        return pltpu.make_async_remote_copy(
            src_ref=block, dst_ref=dst, send_sem=send, recv_sem=recv,
            device_id=device, device_id_type=pl.DeviceIdType.MESH)

    zero[...] = jnp.zeros_like(zero)

    @pl.loop(0, n)
    def _(p):
        def own(big):
            local_copy(src.at[big, p], quadrant(big, p, my_row, my_col), big, p).start()

            @pl.when(jnp.logical_not(aligned))
            def _():
                local_copy(src.at[p, big], quadrant(big, p, my_col, my_row), big, p).start()

        def other(big):
            remote(src.at[big, p], quadrant(big, p, my_row, my_col), sib_sem.at[p, lax.div(big, 2)], block_send_sem, sibling).start()

            @pl.when(jnp.logical_not(aligned))
            def _():
                remote(src.at[p, big], quadrant(big, p, my_col, my_row), sib_sem.at[p, lax.div(big, 2)], block_send_sem, sibling).start()

        own_loop(p, own)
        other_loop(p, other)

        @pl.when(aligned)
        def _():
            @pl.loop(p, n)
            def _(big):
                remote(src.at[big, p], quadrant(big, p, my_row, my_col), nbr_sem.at[p, lax.div(big, 2)], block_send_sem,
                       {"col": 1 - my_col, "row": lax.rem(big, 2)}).start()

    @pl.loop(0, n)
    def _(p):
        @pl.loop(0, p)
        def _(big):
            pltpu.make_async_copy(zero, out.at[big, p], zero_sem).start()

    def wait_blocks(count, sem):
        ref = tiles.at[pl.ds(0, count * NB // 2), :]
        pltpu.make_async_copy(ref, ref, sem).wait()

    def arrive(p):
        def own(big):
            half = lax.div(big, 2)
            wait_blocks(1, nbr_sem.at[p, half])

            @pl.when(aligned)
            def _():
                wait_blocks(1, loc_sem.at[p, half])
                wait_blocks(2, sib_sem.at[p, half])

            @pl.when(jnp.logical_not(aligned))
            def _():
                wait_blocks(2, loc_sem.at[p, half])
                wait_blocks(1, sib_sem.at[p, half])

        own_loop(p, own)

        def turn(big):
            for c in range(2):
                @pl.when(my_col == c)
                def _():
                    rows = pl.ds(tile_row(big, p) + c * NB, NB)
                    lanes = slice((1 - c) * NB, (2 - c) * NB)
                    tiles[rows, lanes] = tiles[rows, lanes].T

        own_loop(p, turn)

    def factor(which):
        def store(t, up, inv):
            upper[SUB * t:SUB * (t + 1), :] = up
            blk_inv[which, SUB * t:SUB * (t + 1), :] = inv

        factor_block(lambda t: blk[SUB * t:SUB * (t + 1), :], store)

    def parts(ref_row):
        row = pl.multiple_of(ref_row * W, W)
        return tuple(ref[pl.ds(row, W), :] for ref in (hi, mid, low))

    def keep_parts(big, value):
        row = pl.multiple_of(big * W, W)
        for ref, val in zip((hi, mid, low), split3(value)):
            ref[pl.ds(row, W), :] = val

    def diag_copy(s):
        return remote(tile_ref(s, s), tile_ref(s, s), diag_sem.at[s], diag_send_sem.at[s], sibling)

    def panel_copy(big, s):
        return remote(tile_ref(big, s), tile_ref(big, s), panel_sem.at[s, lax.div(big, 2)], panel_send_sem.at[lax.div(big, 2)], sibling)

    def update(big, p, rhs):
        trow = tile_row(big, p)
        tiles[pl.ds(trow, W), :] = tiles[pl.ds(trow, W), :] - six(dot_nt, parts(big), rhs)

    def own(s):
        return lax.rem(s, 2) == my_row

    arrive(0)

    @pl.when(own(0))
    def _():
        diag_copy(0).start()

    @pl.loop(0, n)
    def _(s):
        @pl.when(own(s))
        def _():
            diag_copy(s).wait_send()

        @pl.when(jnp.logical_not(own(s)))
        def _():
            diag_copy(s).wait_recv()

        row = tile_row(s, s)
        top, bottom = pl.ds(row, NB), pl.ds(row + NB, NB)

        @pl.loop(0, 2)
        def _(half):
            @pl.when(half == 0)
            def _():
                blk[...] = tiles[top, 0:NB]

            @pl.when(half == 1)
            def _():
                below = six(dot_nt, split3(tiles[bottom, 0:NB]), split3(blk_inv[0]))
                tiles[bottom, 0:NB] = below
                pieces = split3(below)
                blk[...] = tiles[bottom, NB:W] - six(dot_nt, pieces, pieces)

            factor(half)

            @pl.when(half == 0)
            def _():
                tiles[top, 0:NB] = upper[...].T

            @pl.when(half == 1)
            def _():
                tiles[bottom, NB:W] = upper[...].T

        tiles[top, NB:W] = jnp.zeros((NB, NB), F32)
        l21_parts = split3(tiles[bottom, 0:NB])
        inv1, inv2 = split3(blk_inv[0]), split3(blk_inv[1])
        cross = six(dot_nn, split3(six(dot_nn, inv2, l21_parts)), inv1)
        for part in range(3):
            invs[part, 0:NB, 0:NB] = inv1[part]
            invs[part, NB:W, NB:W] = inv2[part]
            invs[part, 0:NB, NB:W] = jnp.zeros((NB, NB), BF16)
        for part, val in enumerate(split3(-cross)):
            invs[part, NB:W, 0:NB] = val

        def solve(big):
            trow = tile_row(big, s)
            sol = six(dot_nt, split3(tiles[pl.ds(trow, W), :]), (invs[0], invs[1], invs[2]))
            tiles[pl.ds(trow, W), :] = sol
            panel_copy(big, s).start()
            keep_parts(big, sol)

        own_loop(s + 1, solve)

        @pl.when(jnp.logical_and(s == 0, s + 1 < n))
        def _():
            arrive(1)

        @pl.when(jnp.logical_and(own(s + 1), s + 1 < n))
        def _():
            update(s + 1, s + 1, parts(s + 1))
            diag_copy(s + 1).start()

        other_loop(s + 1, lambda big: panel_copy(big, s).wait_recv())
        other_loop(s + 1, lambda big: keep_parts(big, tiles[pl.ds(tile_row(big, s), W), :]))

        @pl.loop(s, n)
        def _(big):
            pltpu.make_async_copy(quadrant(big, s, my_row, my_col), out.at[big, s], out_sem).start()

        @pl.loop(s + 1, n)
        def _(p):
            @pl.when(jnp.logical_and(s == 0, p > 1))
            def _():
                arrive(p)

            first, count = own_tiles(p)
            done = jnp.logical_and(p == s + 1, own(p)).astype(jnp.int32)
            first = first + 2 * done
            count = count - done

            @pl.loop(0, lax.div(count, 2))
            def _(q):
                rhs = parts(p)
                for j in range(2):
                    update(first + 4 * q + 2 * j, p, rhs)

            @pl.when(lax.rem(count, 2) == 1)
            def _():
                update(first + 2 * (count - 1), p, parts(p))

        own_loop(s + 1, lambda big: panel_copy(big, s).wait_send())

    for r in range(2):
        others = sum((n - p + 1 - (p + 1 + r) % 2) // 2 for p in range(n))

        @pl.when(jnp.logical_and(my_row == r, aligned))
        def _():
            wait_blocks(others + n * (n + 1) // 2, block_send_sem)

        @pl.when(jnp.logical_and(my_row == r, jnp.logical_not(aligned)))
        def _():
            wait_blocks(2 * others, block_send_sem)

    wait_blocks(n * (n + 1) // 2, out_sem)
    wait_blocks(n * (n - 1) // 2, zero_sem)


def solution(mesh):
    grid_spec = P(("b", "row"), "col")

    def local_factor(a_loc):
        n = a_loc.shape[0]
        W = 2 * NB
        dma = pltpu.SemaphoreType.DMA
        return pl.pallas_call(
            functools.partial(kernel, n),
            out_shape=jax.ShapeDtypeStruct(a_loc.shape, F32),
            in_specs=[pl.BlockSpec(memory_space=pl.ANY)],
            out_specs=pl.BlockSpec(memory_space=pl.ANY),
            scratch_shapes=[
                pltpu.VMEM((n * (n + 1) // 2 * W, W), F32),
                pltpu.VMEM((n * W, W), BF16),
                pltpu.VMEM((n * W, W), BF16),
                pltpu.VMEM((n * W, W), BF16),
                pltpu.VMEM((3, W, W), BF16),
                pltpu.VMEM((NB, NB), F32),
                pltpu.VMEM((NB, NB), F32),
                pltpu.VMEM((2, NB, NB), F32),
                pltpu.VMEM((NB, NB), F32),
                dma((n, n // 2)), dma((n, n // 2)), dma((n, n // 2)), dma((n, n // 2)), dma((n,)), dma((n,)),
                dma, dma((n // 2,)), dma, dma,
            ],
            compiler_params=pltpu.CompilerParams(
                vmem_limit_bytes=60 << 20, collective_id=0, has_side_effects=True),
        )(a_loc)

    return jax.shard_map(local_factor, mesh=mesh, in_specs=grid_spec, out_specs=grid_spec, check_vma=False)
```

```python
import functools

import jax
import jax.numpy as jnp
from jax import lax
from jax.experimental import pallas as pl
from jax.experimental.pallas import tpu as pltpu
from jax.sharding import PartitionSpec as P

NB = 128
SUB = 8
F32 = jnp.float32
BF16 = jnp.bfloat16


def split3(x):
    hi = x.astype(BF16)
    rest = x - hi.astype(F32)
    mid = rest.astype(BF16)
    low = (rest - mid.astype(F32)).astype(BF16)
    return hi, mid, low


def dot_nt(a, b):
    return lax.dot_general(a, b, (((1,), (1,)), ((), ())), preferred_element_type=F32)


def dot_nn(a, b):
    return lax.dot_general(a, b, (((1,), (0,)), ((), ())), preferred_element_type=F32)


def six(dot, a, b):
    ah, am, al = a
    bh, bm, bl = b
    small = dot(al, bh) + dot(ah, bl) + dot(am, bm)
    return (small + (dot(am, bh) + dot(ah, bm))) + dot(ah, bh)


def spread_row(x, k):
    return jnp.broadcast_to(x[k:k + 1, :], (SUB, NB))


def spread_cols(x, first):
    return [jnp.broadcast_to(x[:, first + c:first + c + 1], (SUB, NB)) for c in range(SUB)]


def factor_block(load, store):
    steps = NB // SUB
    sub = lax.broadcasted_iota(jnp.int32, (SUB, NB), 0)
    lane = lax.broadcasted_iota(jnp.int32, (SUB, NB), 1)
    rows = [[load(t), jnp.where(lane == sub + SUB * t, 1.0, 0.0).astype(F32)] for t in range(steps)]
    main = spread_cols(rows[0][0], 0)
    ext = spread_cols(rows[1][0], 0)
    for t in range(steps):
        fac, inv = rows[t]
        fac_rows, inv_rows, below = [], [], []
        for k in range(SUB):
            inv_root = lax.rsqrt(spread_row(main[k], k))
            scaled = main[k] * inv_root
            scaled_ext = ext[k] * inv_root if t + 1 < steps else None
            below.append(scaled_ext)
            for c in range(k + 1, SUB):
                factor_c = spread_row(scaled, c)
                main[c] = main[c] - scaled * factor_c
                if t + 1 < steps:
                    ext[c] = ext[c] - scaled_ext * factor_c
            mult = jnp.where(sub > k, scaled, 0.0)
            fac_row = spread_row(fac, k) * inv_root
            inv_row = spread_row(inv, k) * inv_root
            fac = jnp.where(sub == k, fac_row, fac - mult * fac_row)
            inv = jnp.where(sub == k, inv_row, inv - mult * inv_row)
            fac_rows.append(fac_row)
            inv_rows.append(inv_row)
        store(t, jnp.where(lane >= sub + SUB * t, fac, 0.0), jnp.where(lane <= sub + SUB * t, inv, 0.0))
        if t + 1 == steps:
            break
        s = t + 1
        next_main = spread_cols(rows[s][0], SUB * s)
        for k in range(SUB):
            rows[s][0] = rows[s][0] - below[k] * fac_rows[k]
            rows[s][1] = rows[s][1] - below[k] * inv_rows[k]
            for c in range(SUB):
                next_main[c] = next_main[c] - below[k] * spread_row(below[k], c)
        if s + 1 < steps:
            next_ext = spread_cols(rows[s + 1][0], SUB * s)
            for q in range(t + 2, steps):
                for k in range(SUB):
                    col = jnp.take_along_axis(fac_rows[k], sub + SUB * q, axis=1)
                    rows[q][0] = rows[q][0] - col * fac_rows[k]
                    rows[q][1] = rows[q][1] - col * inv_rows[k]
                    if q == t + 2:
                        for c in range(SUB):
                            next_ext[c] = next_ext[c] - col * spread_row(below[k], c)
            ext = next_ext
        main = next_main


def kernel(n, src, out, tiles, hi, mid, low, invs, upper, blk, blk_inv, zero,
           loc_sem, sib_sem, nbr_sem, panel_sem, diag_sem, diag_send_sem, block_send_sem, panel_send_sem,
           out_sem, zero_sem):
    W = 2 * NB
    my_row = lax.axis_index("row")
    my_col = lax.axis_index("col")
    sibling = {"row": 1 - my_row}
    aligned = my_row == my_col
    num_own = n // 2

    barrier = pltpu.get_barrier_semaphore()
    pl.semaphore_signal(barrier, inc=1, device_id=sibling, device_id_type=pl.DeviceIdType.MESH)
    for core in range(2):
        pl.semaphore_signal(barrier, inc=1, device_id={"col": 1 - my_col, "row": core},
                            device_id_type=pl.DeviceIdType.MESH)
    pl.semaphore_wait(barrier, 3)

    def tile_row(big, p):
        return pl.multiple_of((p * n - (p * (p - 1)) // 2 + big - p) * W, W)

    def quadrant(big, p, r, c):
        return tiles.at[pl.ds(pl.multiple_of(tile_row(big, p) + r * NB, NB), NB), pl.ds(pl.multiple_of(c * NB, NB), NB)]

    def tile_ref(big, p):
        return tiles.at[pl.ds(tile_row(big, p), W), :]

    def first_own(p):
        return p + lax.rem(p + my_row, 2)

    def first_other(p):
        return p + lax.rem(p + 1 + my_row, 2)

    def own_tiles(p):
        first = first_own(p)
        return first, lax.div(n + 1 - first, 2)

    def other_tiles(p):
        first = first_other(p)
        return first, lax.div(n + 1 - first, 2)

    def own_loop(p, fn):
        first, count = own_tiles(p)

        @pl.loop(0, count)
        def _(q):
            fn(first + 2 * q)

    def other_loop(p, fn):
        first, count = other_tiles(p)

        @pl.loop(0, count)
        def _(q):
            fn(first + 2 * q)

    def local_copy(block, dst, big, p):
        return pltpu.make_async_copy(block, dst, loc_sem.at[p, lax.div(big, 2)])

    def remote(block, dst, recv, send, device):
        return pltpu.make_async_remote_copy(
            src_ref=block, dst_ref=dst, send_sem=send, recv_sem=recv,
            device_id=device, device_id_type=pl.DeviceIdType.MESH)

    zero[...] = jnp.zeros_like(zero)

    @pl.loop(0, n)
    def _(p):
        def own(big):
            local_copy(src.at[big, p], quadrant(big, p, my_row, my_col), big, p).start()

            @pl.when(jnp.logical_not(aligned))
            def _():
                local_copy(src.at[p, big], quadrant(big, p, my_col, my_row), big, p).start()

        def other(big):
            remote(src.at[big, p], quadrant(big, p, my_row, my_col), sib_sem.at[p, lax.div(big, 2)], block_send_sem, sibling).start()

            @pl.when(jnp.logical_not(aligned))
            def _():
                remote(src.at[p, big], quadrant(big, p, my_col, my_row), sib_sem.at[p, lax.div(big, 2)], block_send_sem, sibling).start()

        own_loop(p, own)
        other_loop(p, other)

        @pl.when(aligned)
        def _():
            @pl.loop(p, n)
            def _(big):
                remote(src.at[big, p], quadrant(big, p, my_row, my_col), nbr_sem.at[p, lax.div(big, 2)], block_send_sem,
                       {"col": 1 - my_col, "row": lax.rem(big, 2)}).start()

    @pl.loop(0, n)
    def _(p):
        @pl.loop(0, p)
        def _(big):
            pltpu.make_async_copy(zero, out.at[big, p], zero_sem).start()

    def wait_blocks(count, sem):
        ref = tiles.at[pl.ds(0, count * NB // 2), :]
        pltpu.make_async_copy(ref, ref, sem).wait()

    def arrive(p):
        def own(big):
            half = lax.div(big, 2)
            wait_blocks(1, nbr_sem.at[p, half])

            @pl.when(aligned)
            def _():
                wait_blocks(1, loc_sem.at[p, half])
                wait_blocks(2, sib_sem.at[p, half])

            @pl.when(jnp.logical_not(aligned))
            def _():
                wait_blocks(2, loc_sem.at[p, half])
                wait_blocks(1, sib_sem.at[p, half])

        own_loop(p, own)

        def turn(big):
            for c in range(2):
                @pl.when(my_col == c)
                def _():
                    rows = pl.ds(tile_row(big, p) + c * NB, NB)
                    lanes = slice((1 - c) * NB, (2 - c) * NB)
                    tiles[rows, lanes] = tiles[rows, lanes].T

        own_loop(p, turn)

    def factor(which):
        def store(t, up, inv):
            upper[SUB * t:SUB * (t + 1), :] = up
            blk_inv[which, SUB * t:SUB * (t + 1), :] = inv

        factor_block(lambda t: blk[SUB * t:SUB * (t + 1), :], store)

    def parts(ref_row):
        row = pl.multiple_of(ref_row * W, W)
        return tuple(ref[pl.ds(row, W), :] for ref in (hi, mid, low))

    def keep_parts(big, value):
        row = pl.multiple_of(big * W, W)
        for ref, val in zip((hi, mid, low), split3(value)):
            ref[pl.ds(row, W), :] = val

    def diag_copy(s):
        return remote(tile_ref(s, s), tile_ref(s, s), diag_sem.at[s], diag_send_sem.at[s], sibling)

    def panel_copy(big, s):
        return remote(tile_ref(big, s), tile_ref(big, s), panel_sem.at[s, lax.div(big, 2)], panel_send_sem.at[lax.div(big, 2)], sibling)

    def update(big, p, rhs):
        trow = tile_row(big, p)
        tiles[pl.ds(trow, W), :] = tiles[pl.ds(trow, W), :] - six(dot_nt, parts(big), rhs)

    def own(s):
        return lax.rem(s, 2) == my_row

    arrive(0)

    @pl.when(own(0))
    def _():
        diag_copy(0).start()

    @pl.loop(0, n)
    def _(s):
        @pl.when(own(s))
        def _():
            diag_copy(s).wait_send()

        @pl.when(jnp.logical_not(own(s)))
        def _():
            diag_copy(s).wait_recv()

        row = tile_row(s, s)
        top, bottom = pl.ds(row, NB), pl.ds(row + NB, NB)

        @pl.loop(0, 2)
        def _(half):
            @pl.when(half == 0)
            def _():
                blk[...] = tiles[top, 0:NB]

            @pl.when(half == 1)
            def _():
                below = six(dot_nt, split3(tiles[bottom, 0:NB]), split3(blk_inv[0]))
                tiles[bottom, 0:NB] = below
                pieces = split3(below)
                blk[...] = tiles[bottom, NB:W] - six(dot_nt, pieces, pieces)

            factor(half)

            @pl.when(half == 0)
            def _():
                tiles[top, 0:NB] = upper[...].T

            @pl.when(half == 1)
            def _():
                tiles[bottom, NB:W] = upper[...].T

        tiles[top, NB:W] = jnp.zeros((NB, NB), F32)
        l21_parts = split3(tiles[bottom, 0:NB])
        inv1, inv2 = split3(blk_inv[0]), split3(blk_inv[1])
        cross = six(dot_nn, split3(six(dot_nn, inv2, l21_parts)), inv1)
        for part in range(3):
            invs[part, 0:NB, 0:NB] = inv1[part]
            invs[part, NB:W, NB:W] = inv2[part]
            invs[part, 0:NB, NB:W] = jnp.zeros((NB, NB), BF16)
        for part, val in enumerate(split3(-cross)):
            invs[part, NB:W, 0:NB] = val

        def solve(big):
            trow = tile_row(big, s)
            sol = six(dot_nt, split3(tiles[pl.ds(trow, W), :]), (invs[0], invs[1], invs[2]))
            tiles[pl.ds(trow, W), :] = sol
            panel_copy(big, s).start()
            keep_parts(big, sol)

        own_loop(s + 1, solve)

        @pl.when(jnp.logical_and(s == 0, s + 1 < n))
        def _():
            arrive(1)

        @pl.when(jnp.logical_and(own(s + 1), s + 1 < n))
        def _():
            update(s + 1, s + 1, parts(s + 1))
            diag_copy(s + 1).start()

        other_loop(s + 1, lambda big: panel_copy(big, s).wait_recv())
        other_loop(s + 1, lambda big: keep_parts(big, tiles[pl.ds(tile_row(big, s), W), :]))

        @pl.loop(s, n)
        def _(big):
            pltpu.make_async_copy(quadrant(big, s, my_row, my_col), out.at[big, s], out_sem).start()

        @pl.loop(s + 1, n)
        def _(p):
            @pl.when(jnp.logical_and(s == 0, p > 1))
            def _():
                arrive(p)

            first, count = own_tiles(p)
            done = jnp.logical_and(p == s + 1, own(p)).astype(jnp.int32)
            first = first + 2 * done
            count = count - done

            @pl.loop(0, lax.div(count, 2))
            def _(q):
                rhs = parts(p)
                for j in range(2):
                    update(first + 4 * q + 2 * j, p, rhs)

            @pl.when(lax.rem(count, 2) == 1)
            def _():
                update(first + 2 * (count - 1), p, parts(p))

        own_loop(s + 1, lambda big: panel_copy(big, s).wait_send())

    for r in range(2):
        others = sum((n - p + 1 - (p + 1 + r) % 2) // 2 for p in range(n))

        @pl.when(jnp.logical_and(my_row == r, aligned))
        def _():
            wait_blocks(others + n * (n + 1) // 2, block_send_sem)

        @pl.when(jnp.logical_and(my_row == r, jnp.logical_not(aligned)))
        def _():
            wait_blocks(2 * others, block_send_sem)

    wait_blocks(n * (n + 1) // 2, out_sem)
    wait_blocks(n * (n - 1) // 2, zero_sem)


def solution(mesh):
    grid_spec = P(("b", "row"), "col")

    def local_factor(a_loc):
        n = a_loc.shape[0]
        W = 2 * NB
        dma = pltpu.SemaphoreType.DMA
        return pl.pallas_call(
            functools.partial(kernel, n),
            out_shape=jax.ShapeDtypeStruct(a_loc.shape, F32),
            in_specs=[pl.BlockSpec(memory_space=pl.ANY)],
            out_specs=pl.BlockSpec(memory_space=pl.ANY),
            scratch_shapes=[
                pltpu.VMEM((n * (n + 1) // 2 * W, W), F32),
                pltpu.VMEM((n * W, W), BF16),
                pltpu.VMEM((n * W, W), BF16),
                pltpu.VMEM((n * W, W), BF16),
                pltpu.VMEM((3, W, W), BF16),
                pltpu.VMEM((NB, NB), F32),
                pltpu.VMEM((NB, NB), F32),
                pltpu.VMEM((2, NB, NB), F32),
                pltpu.VMEM((NB, NB), F32),
                dma((n, n // 2)), dma((n, n // 2)), dma((n, n // 2)), dma((n, n // 2)), dma((n,)), dma((n,)),
                dma, dma((n // 2,)), dma, dma,
            ],
            compiler_params=pltpu.CompilerParams(
                vmem_limit_bytes=60 << 20, collective_id=0, has_side_effects=True),
        )(a_loc)

    return jax.shard_map(local_factor, mesh=mesh, in_specs=grid_spec, out_specs=grid_spec, check_vma=False)
```

```python
import functools

import jax
import jax.numpy as jnp
from jax import lax
from jax.experimental import pallas as pl
from jax.experimental.pallas import tpu as pltpu
from jax.sharding import PartitionSpec as P

NB = 128
SUB = 8
F32 = jnp.float32
BF16 = jnp.bfloat16


def split3(x):
    hi = x.astype(BF16)
    rest = x - hi.astype(F32)
    mid = rest.astype(BF16)
    low = (rest - mid.astype(F32)).astype(BF16)
    return hi, mid, low


def dot_nt(a, b):
    return lax.dot_general(a, b, (((1,), (1,)), ((), ())), preferred_element_type=F32)


def dot_nn(a, b):
    return lax.dot_general(a, b, (((1,), (0,)), ((), ())), preferred_element_type=F32)


def six(dot, a, b):
    ah, am, al = a
    bh, bm, bl = b
    small = dot(al, bh) + dot(ah, bl) + dot(am, bm)
    return (small + (dot(am, bh) + dot(ah, bm))) + dot(ah, bh)


def spread_row(x, k):
    return jnp.broadcast_to(x[k:k + 1, :], (SUB, NB))


def spread_cols(x, first):
    return [jnp.broadcast_to(x[:, first + c:first + c + 1], (SUB, NB)) for c in range(SUB)]


def factor_block(load, store):
    steps = NB // SUB
    sub = lax.broadcasted_iota(jnp.int32, (SUB, NB), 0)
    lane = lax.broadcasted_iota(jnp.int32, (SUB, NB), 1)
    rows = [[load(t), jnp.where(lane == sub + SUB * t, 1.0, 0.0).astype(F32)] for t in range(steps)]
    main = spread_cols(rows[0][0], 0)
    ext = spread_cols(rows[1][0], 0)
    for t in range(steps):
        fac, inv = rows[t]
        fac_rows, inv_rows, below = [], [], []
        for k in range(SUB):
            inv_root = lax.rsqrt(spread_row(main[k], k))
            scaled = main[k] * inv_root
            scaled_ext = ext[k] * inv_root if t + 1 < steps else None
            below.append(scaled_ext)
            for c in range(k + 1, SUB):
                factor_c = spread_row(scaled, c)
                main[c] = main[c] - scaled * factor_c
                if t + 1 < steps:
                    ext[c] = ext[c] - scaled_ext * factor_c
            mult = jnp.where(sub > k, scaled, 0.0)
            fac_row = spread_row(fac, k) * inv_root
            inv_row = spread_row(inv, k) * inv_root
            fac = jnp.where(sub == k, fac_row, fac - mult * fac_row)
            inv = jnp.where(sub == k, inv_row, inv - mult * inv_row)
            fac_rows.append(fac_row)
            inv_rows.append(inv_row)
        store(t, jnp.where(lane >= sub + SUB * t, fac, 0.0), jnp.where(lane <= sub + SUB * t, inv, 0.0))
        if t + 1 == steps:
            break
        s = t + 1
        next_main = spread_cols(rows[s][0], SUB * s)
        for k in range(SUB):
            rows[s][0] = rows[s][0] - below[k] * fac_rows[k]
            rows[s][1] = rows[s][1] - below[k] * inv_rows[k]
            for c in range(SUB):
                next_main[c] = next_main[c] - below[k] * spread_row(below[k], c)
        if s + 1 < steps:
            next_ext = spread_cols(rows[s + 1][0], SUB * s)
            for q in range(t + 2, steps):
                for k in range(SUB):
                    col = jnp.take_along_axis(fac_rows[k], sub + SUB * q, axis=1)
                    rows[q][0] = rows[q][0] - col * fac_rows[k]
                    rows[q][1] = rows[q][1] - col * inv_rows[k]
                    if q == t + 2:
                        for c in range(SUB):
                            next_ext[c] = next_ext[c] - col * spread_row(below[k], c)
            ext = next_ext
        main = next_main


def kernel(n, src, out, tiles, hi, mid, low, invs, linv, upper, blk, blk_inv, zero,
           loc_sem, sib_sem, nbr_sem, twin_sem, panel_sem, diag_sem, diag_send_sem, inv_sem, inv_send_sem, block_send_sem, panel_send_sem,
           out_sem, zero_sem):
    W = 2 * NB
    my_row = lax.axis_index("row")
    my_col = lax.axis_index("col")
    my_rep = lax.axis_index("rep")
    sibling = {"row": 1 - my_row}
    twin = {"rep": 1 - my_rep}
    aligned = my_row == my_col
    num_own = n // 2

    barrier = pltpu.get_barrier_semaphore()
    pl.semaphore_signal(barrier, inc=1, device_id=sibling, device_id_type=pl.DeviceIdType.MESH)
    for core in range(2):
        pl.semaphore_signal(barrier, inc=1, device_id={"col": 1 - my_col, "row": core},
                            device_id_type=pl.DeviceIdType.MESH)
    pl.semaphore_signal(barrier, inc=1, device_id=twin, device_id_type=pl.DeviceIdType.MESH)
    pl.semaphore_wait(barrier, 4)

    def tile_row(big, p):
        return pl.multiple_of((p * n - (p * (p - 1)) // 2 + big - p) * W, W)

    def quadrant(big, p, r, c):
        return tiles.at[pl.ds(pl.multiple_of(tile_row(big, p) + r * NB, NB), NB), pl.ds(pl.multiple_of(c * NB, NB), NB)]

    def tile_ref(big, p):
        return tiles.at[pl.ds(tile_row(big, p), W), :]

    def first_own(p):
        return p + lax.rem(p + my_row, 2)

    def first_other(p):
        return p + lax.rem(p + 1 + my_row, 2)

    def own_tiles(p):
        first = first_own(p)
        return first, lax.div(n + 1 - first, 2)

    def other_tiles(p):
        first = first_other(p)
        return first, lax.div(n + 1 - first, 2)

    def own_loop(p, fn):
        first, count = own_tiles(p)

        @pl.loop(0, count)
        def _(q):
            fn(first + 2 * q)

    def other_loop(p, fn):
        first, count = other_tiles(p)

        @pl.loop(0, count)
        def _(q):
            fn(first + 2 * q)

    def by_x(big, p):
        return lax.rem(lax.div(big, 2) + p, 2) == my_rep

    def local_copy(block, dst, big, p):
        return pltpu.make_async_copy(block, dst, loc_sem.at[p, lax.div(big, 2)])

    def remote(block, dst, recv, send, device):
        return pltpu.make_async_remote_copy(
            src_ref=block, dst_ref=dst, send_sem=send, recv_sem=recv,
            device_id=device, device_id_type=pl.DeviceIdType.MESH)

    zero[...] = jnp.zeros_like(zero)

    @pl.loop(0, n)
    def _(p):
        def own(big):
            local_copy(src.at[big, p], quadrant(big, p, my_row, my_col), big, p).start()

            @pl.when(jnp.logical_not(aligned))
            def _():
                local_copy(src.at[p, big], quadrant(big, p, my_col, my_row), big, p).start()

        def other(big):
            remote(src.at[big, p], quadrant(big, p, my_row, my_col), sib_sem.at[p, lax.div(big, 2)], block_send_sem, sibling).start()

            @pl.when(jnp.logical_not(aligned))
            def _():
                remote(src.at[p, big], quadrant(big, p, my_col, my_row), sib_sem.at[p, lax.div(big, 2)], block_send_sem, sibling).start()

        own_loop(p, own)
        other_loop(p, other)

        @pl.when(aligned)
        def _():
            @pl.loop(p, n)
            def _(big):
                @pl.when(by_x(big, p))
                def _():
                    remote(src.at[big, p], quadrant(big, p, my_row, my_col), nbr_sem.at[p, lax.div(big, 2)],
                           block_send_sem, {"col": 1 - my_col, "row": lax.rem(big, 2)}).start()

    @pl.loop(0, n)
    def _(p):
        @pl.loop(0, p)
        def _(big):
            pltpu.make_async_copy(zero, out.at[big, p], zero_sem).start()

    def wait_blocks(count, sem):
        ref = tiles.at[pl.ds(0, count * NB // 2), :]
        pltpu.make_async_copy(ref, ref, sem).wait()

    def twin_copy(big, p):
        half = lax.div(big, 2)
        block = quadrant(big, p, 1 - my_col, 1 - my_col)
        return remote(block, block, nbr_sem.at[p, half], twin_sem.at[lax.rem(p, 4), half], twin)

    def forward(p):
        def one(big):
            @pl.when(by_x(big, p))
            def _():
                wait_blocks(1, nbr_sem.at[p, lax.div(big, 2)])
                twin_copy(big, p).start()

        own_loop(p, one)

    def arrive(p):
        def own(big):
            half = lax.div(big, 2)

            @pl.when(by_x(big, p))
            def _():
                twin_copy(big, p).wait_send()

            @pl.when(jnp.logical_not(by_x(big, p)))
            def _():
                wait_blocks(1, nbr_sem.at[p, half])

            @pl.when(aligned)
            def _():
                wait_blocks(1, loc_sem.at[p, half])
                wait_blocks(2, sib_sem.at[p, half])

            @pl.when(jnp.logical_not(aligned))
            def _():
                wait_blocks(2, loc_sem.at[p, half])
                wait_blocks(1, sib_sem.at[p, half])

        own_loop(p, own)

        def turn(big):
            for c in range(2):
                @pl.when(my_col == c)
                def _():
                    rows = pl.ds(tile_row(big, p) + c * NB, NB)
                    lanes = slice((1 - c) * NB, (2 - c) * NB)
                    tiles[rows, lanes] = tiles[rows, lanes].T

        own_loop(p, turn)

    def factor(which):
        def store(t, up, inv):
            upper[SUB * t:SUB * (t + 1), :] = up
            blk_inv[which, SUB * t:SUB * (t + 1), :] = inv

        factor_block(lambda t: blk[SUB * t:SUB * (t + 1), :], store)

    def parts(ref_row):
        row = pl.multiple_of(ref_row * W, W)
        return tuple(ref[pl.ds(row, W), :] for ref in (hi, mid, low))

    def keep_parts(big, value):
        row = pl.multiple_of(big * W, W)
        for ref, val in zip((hi, mid, low), split3(value)):
            ref[pl.ds(row, W), :] = val

    def diag_copy(s):
        return remote(tile_ref(s, s), tile_ref(s, s), diag_sem.at[s], diag_send_sem.at[s], sibling)

    def inv_copy(s):
        slot = lax.rem(s, 2)
        return remote(linv.at[slot], linv.at[slot], inv_sem.at[slot], inv_send_sem, sibling)

    def panel_copy(big, s):
        return remote(tile_ref(big, s), tile_ref(big, s), panel_sem.at[s, lax.div(big, 2)], panel_send_sem.at[lax.div(big, 2)], sibling)

    def update(big, p, rhs):
        trow = tile_row(big, p)
        tiles[pl.ds(trow, W), :] = tiles[pl.ds(trow, W), :] - six(dot_nt, parts(big), rhs)

    def own(s):
        return lax.rem(s + 2, 2) == my_row

    def factor_tile(s):
        row = tile_row(s, s)
        top, bottom = pl.ds(row, NB), pl.ds(row + NB, NB)

        @pl.loop(0, 2)
        def _(half):
            @pl.when(half == 0)
            def _():
                blk[...] = tiles[top, 0:NB]

            @pl.when(half == 1)
            def _():
                below = six(dot_nt, split3(tiles[bottom, 0:NB]), split3(blk_inv[0]))
                tiles[bottom, 0:NB] = below
                pieces = split3(below)
                blk[...] = tiles[bottom, NB:W] - six(dot_nt, pieces, pieces)

            factor(half)

            @pl.when(half == 0)
            def _():
                tiles[top, 0:NB] = upper[...].T

            @pl.when(half == 1)
            def _():
                tiles[bottom, NB:W] = upper[...].T

        tiles[top, NB:W] = jnp.zeros((NB, NB), F32)
        l21_parts = split3(tiles[bottom, 0:NB])
        inv1, inv2 = split3(blk_inv[0]), split3(blk_inv[1])
        slot = lax.rem(s, 2)
        linv[slot, NB:W, 0:NB] = -six(dot_nn, split3(six(dot_nn, inv2, l21_parts)), inv1)
        linv[slot, 0:NB, 0:NB] = blk_inv[0]
        linv[slot, NB:W, NB:W] = blk_inv[1]
        linv[slot, 0:NB, NB:W] = jnp.zeros((NB, NB), F32)
        inv_copy(s).start()
        diag_copy(s).start()

    def solve_for(s):
        def solve(big):
            trow = tile_row(big, s)
            sol = six(dot_nt, split3(tiles[pl.ds(trow, W), :]), (invs[0], invs[1], invs[2]))
            tiles[pl.ds(trow, W), :] = sol
            panel_copy(big, s).start()
            keep_parts(big, sol)

        return solve

    def finish(s):
        other_loop(s + 1, lambda big: panel_copy(big, s).wait_recv())
        other_loop(s + 1, lambda big: keep_parts(big, tiles[pl.ds(tile_row(big, s), W), :]))

        @pl.when(jnp.logical_not(own(s)))
        def _():
            diag_copy(s).wait_recv()

        @pl.loop(s, n)
        def _(big):
            pltpu.make_async_copy(quadrant(big, s, my_row, my_col), out.at[big, s], out_sem).start()

        @pl.loop(s + 1, n)
        def _(p):
            @pl.when(jnp.logical_and(s == 0, p > 1))
            def _():
                @pl.when(p + 2 < n)
                def _():
                    forward(p + 2)

                arrive(p)

            first, count = own_tiles(p)
            done = jnp.logical_and(p == s + 1, own(p)).astype(jnp.int32)
            first = first + 2 * done
            count = count - done

            @pl.loop(0, lax.div(count, 2))
            def _(q):
                rhs = parts(p)
                for j in range(2):
                    update(first + 4 * q + 2 * j, p, rhs)

            @pl.when(lax.rem(count, 2) == 1)
            def _():
                update(first + 2 * (count - 1), p, parts(p))

        own_loop(s + 1, lambda big: panel_copy(big, s).wait_send())

    @pl.loop(-1, n)
    def _(s):
        @pl.when(s < 0)
        def _():
            forward(0)
            arrive(0)

        @pl.when(s >= 0)
        def _():
            @pl.when(jnp.logical_not(own(s)))
            def _():
                inv_copy(s).wait_recv()

            for part, val in enumerate(split3(linv[lax.rem(s + 2, 2)])):
                invs[part] = val
            own_loop(s + 1, solve_for(s))

        @pl.when(s == 0)
        def _():
            arrive(1)
            forward(3)

        @pl.when(jnp.logical_and(own(s + 1), s + 1 < n))
        def _():
            @pl.when(s >= 0)
            def _():
                update(s + 1, s + 1, parts(s + 1))

            factor_tile(s + 1)

        @pl.when(s < 0)
        def _():
            forward(1)
            forward(2)

        @pl.when(s >= 0)
        def _():
            finish(s)

        @pl.when(jnp.logical_and(own(s + 1), s + 1 < n))
        def _():
            inv_copy(s + 1).wait_send()
            diag_copy(s + 1).wait_send()

    for r in range(2):
        others = sum((n - p + 1 - (p + 1 + r) % 2) // 2 for p in range(n))
        for copy in range(2):
            crossing = sum((big // 2 + p) % 2 == copy for p in range(n) for big in range(p, n))

            @pl.when(jnp.logical_and(my_row == r, jnp.logical_and(aligned, my_rep == copy)))
            def _():
                wait_blocks(others + crossing, block_send_sem)

        @pl.when(jnp.logical_and(my_row == r, jnp.logical_not(aligned)))
        def _():
            wait_blocks(2 * others, block_send_sem)

    wait_blocks(n * (n + 1) // 2, out_sem)
    wait_blocks(n * (n - 1) // 2, zero_sem)


def solution(mesh):
    grid_spec = P(("b", "row"), "col")

    def local_factor(a_loc):
        n = a_loc.shape[0]
        W = 2 * NB
        dma = pltpu.SemaphoreType.DMA
        return pl.pallas_call(
            functools.partial(kernel, n),
            out_shape=jax.ShapeDtypeStruct(a_loc.shape, F32),
            in_specs=[pl.BlockSpec(memory_space=pl.ANY)],
            out_specs=pl.BlockSpec(memory_space=pl.ANY),
            scratch_shapes=[
                pltpu.VMEM((n * (n + 1) // 2 * W, W), F32),
                pltpu.VMEM((n * W, W), BF16),
                pltpu.VMEM((n * W, W), BF16),
                pltpu.VMEM((n * W, W), BF16),
                pltpu.VMEM((3, W, W), BF16),
                pltpu.VMEM((2, W, W), F32),
                pltpu.VMEM((NB, NB), F32),
                pltpu.VMEM((NB, NB), F32),
                pltpu.VMEM((2, NB, NB), F32),
                pltpu.VMEM((NB, NB), F32),
                dma((n, n // 2)), dma((n, n // 2)), dma((n, n // 2)), dma((4, n // 2)), dma((n, n // 2)), dma((n,)), dma((n,)),
                dma((2,)), dma, dma, dma((n // 2,)), dma, dma,
            ],
            compiler_params=pltpu.CompilerParams(
                vmem_limit_bytes=60 << 20, collective_id=0, has_side_effects=True),
        )(a_loc)

    return jax.shard_map(local_factor, mesh=mesh, in_specs=grid_spec, out_specs=grid_spec, check_vma=False)
```

```python
import functools

import jax
import jax.numpy as jnp
from jax import lax
from jax.experimental import pallas as pl
from jax.experimental.pallas import tpu as pltpu
from jax.sharding import PartitionSpec as P

NB = 128
SUB = 8
F32 = jnp.float32
BF16 = jnp.bfloat16


def split3(x):
    hi = x.astype(BF16)
    rest = x - hi.astype(F32)
    mid = rest.astype(BF16)
    low = (rest - mid.astype(F32)).astype(BF16)
    return hi, mid, low


def dot_nt(a, b):
    return lax.dot_general(a, b, (((1,), (1,)), ((), ())), preferred_element_type=F32)


def dot_nn(a, b):
    return lax.dot_general(a, b, (((1,), (0,)), ((), ())), preferred_element_type=F32)


def six(dot, a, b):
    ah, am, al = a
    bh, bm, bl = b
    small = dot(al, bh) + dot(ah, bl) + dot(am, bm)
    return (small + (dot(am, bh) + dot(ah, bm))) + dot(ah, bh)


def spread_row(x, k):
    return jnp.broadcast_to(x[k:k + 1, :], (SUB, NB))


def spread_cols(x, first):
    return [jnp.broadcast_to(x[:, first + c:first + c + 1], (SUB, NB)) for c in range(SUB)]


def factor_block(load, store):
    steps = NB // SUB
    sub = lax.broadcasted_iota(jnp.int32, (SUB, NB), 0)
    lane = lax.broadcasted_iota(jnp.int32, (SUB, NB), 1)
    rows = [[load(t), jnp.where(lane == sub + SUB * t, 1.0, 0.0).astype(F32)] for t in range(steps)]
    main = spread_cols(rows[0][0], 0)
    ext = spread_cols(rows[1][0], 0)
    for t in range(steps):
        fac, inv = rows[t]
        fac_rows, inv_rows, below = [], [], []
        for k in range(SUB):
            inv_root = lax.rsqrt(spread_row(main[k], k))
            scaled = main[k] * inv_root
            scaled_ext = ext[k] * inv_root if t + 1 < steps else None
            below.append(scaled_ext)
            for c in range(k + 1, SUB):
                factor_c = spread_row(scaled, c)
                main[c] = main[c] - scaled * factor_c
                if t + 1 < steps:
                    ext[c] = ext[c] - scaled_ext * factor_c
            mult = jnp.where(sub > k, scaled, 0.0)
            fac_row = spread_row(fac, k) * inv_root
            inv_row = spread_row(inv, k) * inv_root
            fac = jnp.where(sub == k, fac_row, fac - mult * fac_row)
            inv = jnp.where(sub == k, inv_row, inv - mult * inv_row)
            fac_rows.append(fac_row)
            inv_rows.append(inv_row)
        store(t, jnp.where(lane >= sub + SUB * t, fac, 0.0), jnp.where(lane <= sub + SUB * t, inv, 0.0))
        if t + 1 == steps:
            break
        s = t + 1
        next_main = spread_cols(rows[s][0], SUB * s)
        for k in range(SUB):
            rows[s][0] = rows[s][0] - below[k] * fac_rows[k]
            rows[s][1] = rows[s][1] - below[k] * inv_rows[k]
            for c in range(SUB):
                next_main[c] = next_main[c] - below[k] * spread_row(below[k], c)
        if s + 1 < steps:
            next_ext = spread_cols(rows[s + 1][0], SUB * s)
            for q in range(t + 2, steps):
                for k in range(SUB):
                    col = jnp.take_along_axis(fac_rows[k], sub + SUB * q, axis=1)
                    rows[q][0] = rows[q][0] - col * fac_rows[k]
                    rows[q][1] = rows[q][1] - col * inv_rows[k]
                    if q == t + 2:
                        for c in range(SUB):
                            next_ext[c] = next_ext[c] - col * spread_row(below[k], c)
            ext = next_ext
        main = next_main


def kernel(n, src, out, tiles, hi, mid, low, rhs, invs, linv, upper, blk, blk_inv, zero,
           loc_sem, sib_sem, nbr_sem, twin_sem, panel_sem, diag_sem, diag_send_sem, inv_sem, inv_send_sem, block_send_sem, panel_send_sem,
           out_sem, zero_sem):
    W = 2 * NB
    my_row = lax.axis_index("row")
    my_col = lax.axis_index("col")
    my_rep = lax.axis_index("rep")
    sibling = {"row": 1 - my_row}
    twin = {"rep": 1 - my_rep}
    aligned = my_row == my_col

    barrier = pltpu.get_barrier_semaphore()
    pl.semaphore_signal(barrier, inc=1, device_id=sibling, device_id_type=pl.DeviceIdType.MESH)
    for core in range(2):
        pl.semaphore_signal(barrier, inc=1, device_id={"col": 1 - my_col, "row": core},
                            device_id_type=pl.DeviceIdType.MESH)
    pl.semaphore_signal(barrier, inc=1, device_id=twin, device_id_type=pl.DeviceIdType.MESH)
    pl.semaphore_wait(barrier, 4)

    def tile_row(big, p):
        return pl.multiple_of((p * n - (p * (p - 1)) // 2 + big - p) * W, W)

    def quadrant(big, p, r, c):
        return tiles.at[pl.ds(pl.multiple_of(tile_row(big, p) + r * NB, NB), NB), pl.ds(pl.multiple_of(c * NB, NB), NB)]

    def tile_ref(big, p):
        return tiles.at[pl.ds(tile_row(big, p), W), :]

    def first_own(p):
        return p + lax.rem(p + my_row, 2)

    def first_other(p):
        return p + lax.rem(p + 1 + my_row, 2)

    def own_tiles(p):
        first = first_own(p)
        return first, lax.div(n + 1 - first, 2)

    def other_tiles(p):
        first = first_other(p)
        return first, lax.div(n + 1 - first, 2)

    def own_loop(p, fn):
        first, count = own_tiles(p)

        @pl.loop(0, count)
        def _(q):
            fn(first + 2 * q)

    def other_loop(p, fn):
        first, count = other_tiles(p)

        @pl.loop(0, count)
        def _(q):
            fn(first + 2 * q)

    def by_x(big, p):
        return lax.rem(lax.div(big, 2) + p, 2) == my_rep

    def local_copy(block, dst, big, p):
        return pltpu.make_async_copy(block, dst, loc_sem.at[p, lax.div(big, 2)])

    def remote(block, dst, recv, send, device):
        return pltpu.make_async_remote_copy(
            src_ref=block, dst_ref=dst, send_sem=send, recv_sem=recv,
            device_id=device, device_id_type=pl.DeviceIdType.MESH)

    zero[...] = jnp.zeros_like(zero)

    @pl.loop(0, n)
    def _(p):
        def own(big):
            local_copy(src.at[big, p], quadrant(big, p, my_row, my_col), big, p).start()

            @pl.when(jnp.logical_not(aligned))
            def _():
                local_copy(src.at[p, big], quadrant(big, p, my_col, my_row), big, p).start()

        def other(big):
            remote(src.at[big, p], quadrant(big, p, my_row, my_col), sib_sem.at[p, lax.div(big, 2)], block_send_sem, sibling).start()

            @pl.when(jnp.logical_not(aligned))
            def _():
                remote(src.at[p, big], quadrant(big, p, my_col, my_row), sib_sem.at[p, lax.div(big, 2)], block_send_sem, sibling).start()

        own_loop(p, own)
        other_loop(p, other)

        @pl.when(aligned)
        def _():
            @pl.loop(p, n)
            def _(big):
                @pl.when(by_x(big, p))
                def _():
                    remote(src.at[big, p], quadrant(big, p, my_row, my_col), nbr_sem.at[p, lax.div(big, 2)],
                           block_send_sem, {"col": 1 - my_col, "row": lax.rem(big, 2)}).start()

    @pl.loop(0, n)
    def _(p):
        @pl.loop(0, p)
        def _(big):
            pltpu.make_async_copy(zero, out.at[big, p], zero_sem).start()

    def wait_blocks(count, sem):
        ref = tiles.at[pl.ds(0, count * NB // 2), :]
        pltpu.make_async_copy(ref, ref, sem).wait()

    def twin_copy(big, p):
        half = lax.div(big, 2)
        block = quadrant(big, p, 1 - my_col, 1 - my_col)
        return remote(block, block, nbr_sem.at[p, half], twin_sem.at[lax.rem(p, 4), half], twin)

    def forward(p):
        def one(big):
            @pl.when(by_x(big, p))
            def _():
                wait_blocks(1, nbr_sem.at[p, lax.div(big, 2)])
                twin_copy(big, p).start()

        own_loop(p, one)

    def arrive(p):
        def own(big):
            half = lax.div(big, 2)

            @pl.when(by_x(big, p))
            def _():
                twin_copy(big, p).wait_send()

            @pl.when(jnp.logical_not(by_x(big, p)))
            def _():
                wait_blocks(1, nbr_sem.at[p, half])

            @pl.when(aligned)
            def _():
                wait_blocks(1, loc_sem.at[p, half])
                wait_blocks(2, sib_sem.at[p, half])

            @pl.when(jnp.logical_not(aligned))
            def _():
                wait_blocks(2, loc_sem.at[p, half])
                wait_blocks(1, sib_sem.at[p, half])

        own_loop(p, own)

        def turn(big):
            for c in range(2):
                @pl.when(my_col == c)
                def _():
                    rows = pl.ds(tile_row(big, p) + c * NB, NB)
                    lanes = slice((1 - c) * NB, (2 - c) * NB)
                    tiles[rows, lanes] = tiles[rows, lanes].T

        own_loop(p, turn)

    def factor(which):
        def store(t, up, inv):
            upper[SUB * t:SUB * (t + 1), :] = up
            blk_inv[which, SUB * t:SUB * (t + 1), :] = inv

        factor_block(lambda t: blk[SUB * t:SUB * (t + 1), :], store)

    def kept_row(s, big):
        half = lax.div(big, 2)
        return pl.multiple_of((half * half + s) * W, W)

    def parts(s, big):
        row = kept_row(s, big)
        return tuple(ref[pl.ds(row, W), :] for ref in (hi, mid, low))

    def keep_parts(s, big, value):
        row = kept_row(s, big)
        for ref, val in zip((hi, mid, low), split3(value)):
            ref[pl.ds(row, W), :] = val

    def diag_copy(s):
        return remote(tile_ref(s, s), tile_ref(s, s), diag_sem.at[s], diag_send_sem.at[s], sibling)

    def inv_copy(s):
        slot = lax.rem(s, 2)
        return remote(linv.at[slot], linv.at[slot], inv_sem.at[slot], inv_send_sem, sibling)

    def panel_copy(big, s):
        return remote(tile_ref(big, s), tile_ref(big, s), panel_sem.at[s, lax.div(big, 2)], panel_send_sem.at[lax.div(big, 2)], sibling)

    def update(s, big, p, right):
        trow = tile_row(big, p)
        tiles[pl.ds(trow, W), :] = tiles[pl.ds(trow, W), :] - six(dot_nt, parts(s, big), right)

    def own(s):
        return lax.rem(s + 2, 2) == my_row

    def factor_tile(s):
        row = tile_row(s, s)
        top, bottom = pl.ds(row, NB), pl.ds(row + NB, NB)

        @pl.loop(0, 2)
        def _(half):
            @pl.when(half == 0)
            def _():
                blk[...] = tiles[top, 0:NB]

            @pl.when(half == 1)
            def _():
                below = six(dot_nt, split3(tiles[bottom, 0:NB]), split3(blk_inv[0]))
                tiles[bottom, 0:NB] = below
                pieces = split3(below)
                blk[...] = tiles[bottom, NB:W] - six(dot_nt, pieces, pieces)

            factor(half)

            @pl.when(half == 0)
            def _():
                tiles[top, 0:NB] = upper[...].T

            @pl.when(half == 1)
            def _():
                tiles[bottom, NB:W] = upper[...].T

        tiles[top, NB:W] = jnp.zeros((NB, NB), F32)
        l21_parts = split3(tiles[bottom, 0:NB])
        inv1, inv2 = split3(blk_inv[0]), split3(blk_inv[1])
        slot = lax.rem(s, 2)
        linv[slot, NB:W, 0:NB] = -six(dot_nn, split3(six(dot_nn, inv2, l21_parts)), inv1)
        linv[slot, 0:NB, 0:NB] = blk_inv[0]
        linv[slot, NB:W, NB:W] = blk_inv[1]
        linv[slot, 0:NB, NB:W] = jnp.zeros((NB, NB), F32)
        inv_copy(s).start()
        diag_copy(s).start()

    def solve_for(s):
        def solve(big):
            trow = tile_row(big, s)
            sol = six(dot_nt, split3(tiles[pl.ds(trow, W), :]), (invs[0], invs[1], invs[2]))
            tiles[pl.ds(trow, W), :] = sol
            panel_copy(big, s).start()
            keep_parts(s, big, sol)

        return solve

    def finish(s):
        other_loop(s + 1, lambda big: panel_copy(big, s).wait_recv())

        @pl.when(jnp.logical_not(own(s)))
        def _():
            diag_copy(s).wait_recv()

        @pl.loop(s, n)
        def _(big):
            pltpu.make_async_copy(quadrant(big, s, my_row, my_col), out.at[big, s], out_sem).start()

        def update_column(p, step, first, count):
            for part, val in enumerate(split3(tiles[pl.ds(tile_row(p, step), W), :])):
                rhs[part] = val

            @pl.loop(0, lax.div(count, 2))
            def _(q):
                for j in range(2):
                    update(step, first + 4 * q + 2 * j, p, (rhs[0], rhs[1], rhs[2]))

            @pl.when(lax.rem(count, 2) == 1)
            def _():
                update(step, first + 2 * (count - 1), p, (rhs[0], rhs[1], rhs[2]))

        @pl.when(s + 1 < n)
        def _():
            first, count = own_tiles(s + 1)
            done = own(s + 1).astype(jnp.int32)
            update_column(s + 1, s, first + 2 * done, count - done)

        @pl.when(s + 2 < n)
        def _():
            @pl.when(s + 4 < n)
            def _():
                forward(s + 4)

            arrive(s + 2)
            first, count = own_tiles(s + 2)

            @pl.loop(0, s + 1)
            def _(step):
                update_column(s + 2, step, first, count)

        own_loop(s + 1, lambda big: panel_copy(big, s).wait_send())

    @pl.loop(-1, n)
    def _(s):
        @pl.when(s < 0)
        def _():
            forward(0)
            arrive(0)

        @pl.when(s >= 0)
        def _():
            @pl.when(jnp.logical_not(own(s)))
            def _():
                inv_copy(s).wait_recv()

            for part, val in enumerate(split3(linv[lax.rem(s + 2, 2)])):
                invs[part] = val
            own_loop(s + 1, solve_for(s))

        @pl.when(s == 0)
        def _():
            arrive(1)
            forward(3)

        @pl.when(jnp.logical_and(own(s + 1), s + 1 < n))
        def _():
            @pl.when(s >= 0)
            def _():
                update(s, s + 1, s + 1, parts(s, s + 1))

            factor_tile(s + 1)

        @pl.when(s < 0)
        def _():
            forward(1)
            forward(2)

        @pl.when(s >= 0)
        def _():
            finish(s)

        @pl.when(jnp.logical_and(own(s + 1), s + 1 < n))
        def _():
            inv_copy(s + 1).wait_send()
            diag_copy(s + 1).wait_send()

    for r in range(2):
        others = sum((n - p + 1 - (p + 1 + r) % 2) // 2 for p in range(n))
        for copy in range(2):
            crossing = sum((big // 2 + p) % 2 == copy for p in range(n) for big in range(p, n))

            @pl.when(jnp.logical_and(my_row == r, jnp.logical_and(aligned, my_rep == copy)))
            def _():
                wait_blocks(others + crossing, block_send_sem)

        @pl.when(jnp.logical_and(my_row == r, jnp.logical_not(aligned)))
        def _():
            wait_blocks(2 * others, block_send_sem)

    wait_blocks(n * (n + 1) // 2, out_sem)
    wait_blocks(n * (n - 1) // 2, zero_sem)


def solution(mesh):
    grid_spec = P(("b", "row"), "col")

    def local_factor(a_loc):
        n = a_loc.shape[0]
        W = 2 * NB
        dma = pltpu.SemaphoreType.DMA
        return pl.pallas_call(
            functools.partial(kernel, n),
            out_shape=jax.ShapeDtypeStruct(a_loc.shape, F32),
            in_specs=[pl.BlockSpec(memory_space=pl.ANY)],
            out_specs=pl.BlockSpec(memory_space=pl.ANY),
            scratch_shapes=[
                pltpu.VMEM((n * (n + 1) // 2 * W, W), F32),
                pltpu.VMEM((n * n // 4 * W, W), BF16),
                pltpu.VMEM((n * n // 4 * W, W), BF16),
                pltpu.VMEM((n * n // 4 * W, W), BF16),
                pltpu.VMEM((3, W, W), BF16),
                pltpu.VMEM((3, W, W), BF16),
                pltpu.VMEM((2, W, W), F32),
                pltpu.VMEM((NB, NB), F32),
                pltpu.VMEM((NB, NB), F32),
                pltpu.VMEM((2, NB, NB), F32),
                pltpu.VMEM((NB, NB), F32),
                dma((n, n // 2)), dma((n, n // 2)), dma((n, n // 2)), dma((4, n // 2)), dma((n, n // 2)), dma((n,)), dma((n,)),
                dma((2,)), dma, dma, dma((n // 2,)), dma, dma,
            ],
            compiler_params=pltpu.CompilerParams(
                vmem_limit_bytes=60 << 20, collective_id=0, has_side_effects=True),
        )(a_loc)

    return jax.shard_map(local_factor, mesh=mesh, in_specs=grid_spec, out_specs=grid_spec, check_vma=False)
```

```python
import functools

import jax
import jax.numpy as jnp
from jax import lax
from jax.experimental import pallas as pl
from jax.experimental.pallas import tpu as pltpu
from jax.sharding import PartitionSpec as P

NB = 128
SUB = 8
F32 = jnp.float32
BF16 = jnp.bfloat16


def split3(x):
    hi = x.astype(BF16)
    rest = x - hi.astype(F32)
    mid = rest.astype(BF16)
    low = (rest - mid.astype(F32)).astype(BF16)
    return hi, mid, low


def dot_nt(a, b):
    return lax.dot_general(a, b, (((1,), (1,)), ((), ())), preferred_element_type=F32)


def dot_nn(a, b):
    return lax.dot_general(a, b, (((1,), (0,)), ((), ())), preferred_element_type=F32)


def six(dot, a, b):
    ah, am, al = a
    bh, bm, bl = b
    small = dot(al, bh) + dot(ah, bl) + dot(am, bm)
    return (small + (dot(am, bh) + dot(ah, bm))) + dot(ah, bh)


def spread_row(x, k):
    return jnp.broadcast_to(x[k:k + 1, :], (SUB, NB))


def spread_cols(x, first):
    return [jnp.broadcast_to(x[:, first + c:first + c + 1], (SUB, NB)) for c in range(SUB)]


def factor_block(load, store):
    steps = NB // SUB
    sub = lax.broadcasted_iota(jnp.int32, (SUB, NB), 0)
    lane = lax.broadcasted_iota(jnp.int32, (SUB, NB), 1)
    rows = [[load(t), jnp.where(lane == sub + SUB * t, 1.0, 0.0).astype(F32)] for t in range(steps)]
    main = spread_cols(rows[0][0], 0)
    ext = spread_cols(rows[1][0], 0)
    for t in range(steps):
        fac, inv = rows[t]
        fac_rows, inv_rows, below = [], [], []
        for k in range(SUB):
            inv_root = lax.rsqrt(spread_row(main[k], k))
            scaled = main[k] * inv_root
            scaled_ext = ext[k] * inv_root if t + 1 < steps else None
            below.append(scaled_ext)
            for c in range(k + 1, SUB):
                factor_c = spread_row(scaled, c)
                main[c] = main[c] - scaled * factor_c
                if t + 1 < steps:
                    ext[c] = ext[c] - scaled_ext * factor_c
            mult = jnp.where(sub > k, scaled, 0.0)
            fac_row = spread_row(fac, k) * inv_root
            inv_row = spread_row(inv, k) * inv_root
            fac = jnp.where(sub == k, fac_row, fac - mult * fac_row)
            inv = jnp.where(sub == k, inv_row, inv - mult * inv_row)
            fac_rows.append(fac_row)
            inv_rows.append(inv_row)
        store(t, jnp.where(lane >= sub + SUB * t, fac, 0.0), jnp.where(lane <= sub + SUB * t, inv, 0.0))
        if t + 1 == steps:
            break
        s = t + 1
        next_main = spread_cols(rows[s][0], SUB * s)
        for k in range(SUB):
            rows[s][0] = rows[s][0] - below[k] * fac_rows[k]
            rows[s][1] = rows[s][1] - below[k] * inv_rows[k]
            for c in range(SUB):
                next_main[c] = next_main[c] - below[k] * spread_row(below[k], c)
        if s + 1 < steps:
            next_ext = spread_cols(rows[s + 1][0], SUB * s)
            for q in range(t + 2, steps):
                for k in range(SUB):
                    col = jnp.take_along_axis(fac_rows[k], sub + SUB * q, axis=1)
                    rows[q][0] = rows[q][0] - col * fac_rows[k]
                    rows[q][1] = rows[q][1] - col * inv_rows[k]
                    if q == t + 2:
                        for c in range(SUB):
                            next_ext[c] = next_ext[c] - col * spread_row(below[k], c)
            ext = next_ext
        main = next_main


def kernel(n, src, out, tiles, hi, mid, low, rhs, invs, linv, upper, blk, blk_inv, zero,
           loc_sem, sib_sem, nbr_sem, twin_sem, panel_sem, diag_sem, diag_send_sem, inv_sem, inv_send_sem, block_send_sem, panel_send_sem,
           out_sem, zero_sem):
    W = 2 * NB
    my_row = lax.axis_index("row")
    my_col = lax.axis_index("col")
    my_rep = lax.axis_index("rep")
    sibling = {"row": 1 - my_row}
    twin = {"rep": 1 - my_rep}
    aligned = my_row == my_col

    barrier = pltpu.get_barrier_semaphore()
    pl.semaphore_signal(barrier, inc=1, device_id=sibling, device_id_type=pl.DeviceIdType.MESH)
    for core in range(2):
        pl.semaphore_signal(barrier, inc=1, device_id={"col": 1 - my_col, "row": core},
                            device_id_type=pl.DeviceIdType.MESH)
    pl.semaphore_signal(barrier, inc=1, device_id=twin, device_id_type=pl.DeviceIdType.MESH)
    pl.semaphore_wait(barrier, 4)

    def tile_row(big, p):
        return pl.multiple_of((p * n - (p * (p - 1)) // 2 + big - p) * W, W)

    def quadrant(big, p, r, c):
        return tiles.at[pl.ds(pl.multiple_of(tile_row(big, p) + r * NB, NB), NB), pl.ds(pl.multiple_of(c * NB, NB), NB)]

    def tile_ref(big, p):
        return tiles.at[pl.ds(tile_row(big, p), W), :]

    def first_own(p):
        return p + lax.rem(p + my_row, 2)

    def first_other(p):
        return p + lax.rem(p + 1 + my_row, 2)

    def own_tiles(p):
        first = first_own(p)
        return first, lax.div(n + 1 - first, 2)

    def other_tiles(p):
        first = first_other(p)
        return first, lax.div(n + 1 - first, 2)

    def own_loop(p, fn):
        first, count = own_tiles(p)

        @pl.loop(0, count)
        def _(q):
            fn(first + 2 * q)

    def other_loop(p, fn):
        first, count = other_tiles(p)

        @pl.loop(0, count)
        def _(q):
            fn(first + 2 * q)

    def by_x(big, p):
        return lax.rem(lax.div(big, 2) + p, 2) == my_rep

    def local_copy(block, dst, big, p):
        return pltpu.make_async_copy(block, dst, loc_sem.at[p, lax.div(big, 2)])

    def remote(block, dst, recv, send, device):
        return pltpu.make_async_remote_copy(
            src_ref=block, dst_ref=dst, send_sem=send, recv_sem=recv,
            device_id=device, device_id_type=pl.DeviceIdType.MESH)

    zero[...] = jnp.zeros_like(zero)

    @pl.loop(0, n)
    def _(p):
        def own(big):
            local_copy(src.at[big, p], quadrant(big, p, my_row, my_col), big, p).start()

            @pl.when(jnp.logical_not(aligned))
            def _():
                local_copy(src.at[p, big], quadrant(big, p, my_col, my_row), big, p).start()

        def other(big):
            remote(src.at[big, p], quadrant(big, p, my_row, my_col), sib_sem.at[p, lax.div(big, 2)], block_send_sem, sibling).start()

            @pl.when(jnp.logical_not(aligned))
            def _():
                remote(src.at[p, big], quadrant(big, p, my_col, my_row), sib_sem.at[p, lax.div(big, 2)], block_send_sem, sibling).start()

        own_loop(p, own)
        other_loop(p, other)

        @pl.when(aligned)
        def _():
            @pl.loop(p, n)
            def _(big):
                @pl.when(by_x(big, p))
                def _():
                    remote(src.at[big, p], quadrant(big, p, my_row, my_col), nbr_sem.at[p, lax.div(big, 2)],
                           block_send_sem, {"col": 1 - my_col, "row": lax.rem(big, 2)}).start()

    @pl.loop(0, n)
    def _(p):
        @pl.loop(0, p)
        def _(big):
            pltpu.make_async_copy(zero, out.at[big, p], zero_sem).start()

    def wait_blocks(count, sem):
        ref = tiles.at[pl.ds(0, count * NB // 2), :]
        pltpu.make_async_copy(ref, ref, sem).wait()

    def twin_copy(big, p):
        half = lax.div(big, 2)
        block = quadrant(big, p, 1 - my_col, 1 - my_col)
        return remote(block, block, nbr_sem.at[p, half], twin_sem.at[lax.rem(p, 4), half], twin)

    def forward(p):
        def one(big):
            @pl.when(by_x(big, p))
            def _():
                wait_blocks(1, nbr_sem.at[p, lax.div(big, 2)])
                twin_copy(big, p).start()

        own_loop(p, one)

    def arrive(p):
        def own(big):
            half = lax.div(big, 2)

            @pl.when(by_x(big, p))
            def _():
                twin_copy(big, p).wait_send()

            @pl.when(jnp.logical_not(by_x(big, p)))
            def _():
                wait_blocks(1, nbr_sem.at[p, half])

            @pl.when(aligned)
            def _():
                wait_blocks(1, loc_sem.at[p, half])
                wait_blocks(2, sib_sem.at[p, half])

            @pl.when(jnp.logical_not(aligned))
            def _():
                wait_blocks(2, loc_sem.at[p, half])
                wait_blocks(1, sib_sem.at[p, half])

        own_loop(p, own)

        def turn(big):
            for c in range(2):
                @pl.when(my_col == c)
                def _():
                    rows = pl.ds(tile_row(big, p) + c * NB, NB)
                    lanes = slice((1 - c) * NB, (2 - c) * NB)
                    tiles[rows, lanes] = tiles[rows, lanes].T

        own_loop(p, turn)

    def factor(which):
        def store(t, up, inv):
            upper[SUB * t:SUB * (t + 1), :] = up
            blk_inv[which, SUB * t:SUB * (t + 1), :] = inv

        factor_block(lambda t: blk[SUB * t:SUB * (t + 1), :], store)

    def kept_row(s, big):
        half = lax.div(big, 2)
        return pl.multiple_of((half * half + s) * W, W)

    def parts(s, big):
        row = kept_row(s, big)
        return tuple(ref[pl.ds(row, W), :] for ref in (hi, mid, low))

    def keep_parts(s, big, value):
        row = kept_row(s, big)
        for ref, val in zip((hi, mid, low), split3(value)):
            ref[pl.ds(row, W), :] = val

    def diag_copy(s):
        return remote(tile_ref(s, s), tile_ref(s, s), diag_sem.at[s], diag_send_sem.at[s], sibling)

    def inv_copy(s):
        slot = lax.rem(s, 2)
        return remote(linv.at[slot], linv.at[slot], inv_sem.at[slot], inv_send_sem, sibling)

    def panel_copy(big, s):
        return remote(tile_ref(big, s), tile_ref(big, s), panel_sem.at[s, lax.div(big, 2)], panel_send_sem.at[lax.div(big, 2)], sibling)

    def update(s, big, p, right):
        trow = tile_row(big, p)
        tiles[pl.ds(trow, W), :] = tiles[pl.ds(trow, W), :] - six(dot_nt, parts(s, big), right)

    def own(s):
        return lax.rem(s + 2, 2) == my_row

    def factor_tile(s):
        row = tile_row(s, s)
        top, bottom = pl.ds(row, NB), pl.ds(row + NB, NB)

        @pl.loop(0, 2)
        def _(half):
            @pl.when(half == 0)
            def _():
                blk[...] = tiles[top, 0:NB]

            @pl.when(half == 1)
            def _():
                below = six(dot_nt, split3(tiles[bottom, 0:NB]), split3(blk_inv[0]))
                tiles[bottom, 0:NB] = below
                pieces = split3(below)
                blk[...] = tiles[bottom, NB:W] - six(dot_nt, pieces, pieces)

            factor(half)

            @pl.when(half == 0)
            def _():
                tiles[top, 0:NB] = upper[...].T

            @pl.when(half == 1)
            def _():
                tiles[bottom, NB:W] = upper[...].T

        tiles[top, NB:W] = jnp.zeros((NB, NB), F32)
        l21_parts = split3(tiles[bottom, 0:NB])
        inv1, inv2 = split3(blk_inv[0]), split3(blk_inv[1])
        slot = lax.rem(s, 2)
        linv[slot, NB:W, 0:NB] = -six(dot_nn, split3(six(dot_nn, inv2, l21_parts)), inv1)
        linv[slot, 0:NB, 0:NB] = blk_inv[0]
        linv[slot, NB:W, NB:W] = blk_inv[1]
        linv[slot, 0:NB, NB:W] = jnp.zeros((NB, NB), F32)
        inv_copy(s).start()
        diag_copy(s).start()

    def solve_for(s):
        def solve(big):
            trow = tile_row(big, s)
            sol = six(dot_nt, split3(tiles[pl.ds(trow, W), :]), (invs[0], invs[1], invs[2]))
            tiles[pl.ds(trow, W), :] = sol
            panel_copy(big, s).start()
            keep_parts(s, big, sol)

        return solve

    def finish(s):
        def update_column(p, step, first, count):
            def tiles_with(right):
                @pl.loop(0, lax.div(count, 2))
                def _(q):
                    value = right()
                    for j in range(2):
                        update(step, first + 4 * q + 2 * j, p, value)

                @pl.when(lax.rem(count, 2) == 1)
                def _():
                    update(step, first + 2 * (count - 1), p, right())

            @pl.when(own(p))
            def _():
                tiles_with(lambda: parts(step, p))

            @pl.when(jnp.logical_not(own(p)))
            def _():
                for part, val in enumerate(split3(tiles[pl.ds(tile_row(p, step), W), :])):
                    rhs[part] = val

                tiles_with(lambda: (rhs[0], rhs[1], rhs[2]))

        @pl.when(s + 2 < n)
        def _():
            @pl.when(s + 4 < n)
            def _():
                forward(s + 4)

            arrive(s + 2)
            first, count = own_tiles(s + 2)

            @pl.loop(0, s)
            def _(step):
                update_column(s + 2, step, first, count)

        other_loop(s + 1, lambda big: panel_copy(big, s).wait_recv())

        @pl.when(jnp.logical_not(own(s)))
        def _():
            diag_copy(s).wait_recv()

        @pl.loop(s, n)
        def _(big):
            pltpu.make_async_copy(quadrant(big, s, my_row, my_col), out.at[big, s], out_sem).start()

        @pl.when(s + 1 < n)
        def _():
            first, count = own_tiles(s + 1)
            done = own(s + 1).astype(jnp.int32)
            update_column(s + 1, s, first + 2 * done, count - done)

        @pl.when(s + 2 < n)
        def _():
            first, count = own_tiles(s + 2)
            update_column(s + 2, s, first, count)

        own_loop(s + 1, lambda big: panel_copy(big, s).wait_send())

    @pl.loop(-1, n)
    def _(s):
        @pl.when(s < 0)
        def _():
            forward(0)
            arrive(0)

        @pl.when(s >= 0)
        def _():
            @pl.when(jnp.logical_not(own(s)))
            def _():
                inv_copy(s).wait_recv()

            for part, val in enumerate(split3(linv[lax.rem(s + 2, 2)])):
                invs[part] = val
            own_loop(s + 1, solve_for(s))

        @pl.when(s == 0)
        def _():
            arrive(1)
            forward(3)

        @pl.when(jnp.logical_and(own(s + 1), s + 1 < n))
        def _():
            @pl.when(s >= 0)
            def _():
                update(s, s + 1, s + 1, parts(s, s + 1))

            factor_tile(s + 1)

        @pl.when(s < 0)
        def _():
            forward(1)
            forward(2)

        @pl.when(s >= 0)
        def _():
            finish(s)

        @pl.when(jnp.logical_and(own(s + 1), s + 1 < n))
        def _():
            inv_copy(s + 1).wait_send()
            diag_copy(s + 1).wait_send()

    for r in range(2):
        others = sum((n - p + 1 - (p + 1 + r) % 2) // 2 for p in range(n))
        for copy in range(2):
            crossing = sum((big // 2 + p) % 2 == copy for p in range(n) for big in range(p, n))

            @pl.when(jnp.logical_and(my_row == r, jnp.logical_and(aligned, my_rep == copy)))
            def _():
                wait_blocks(others + crossing, block_send_sem)

        @pl.when(jnp.logical_and(my_row == r, jnp.logical_not(aligned)))
        def _():
            wait_blocks(2 * others, block_send_sem)

    wait_blocks(n * (n + 1) // 2, out_sem)
    wait_blocks(n * (n - 1) // 2, zero_sem)


def solution(mesh):
    grid_spec = P(("b", "row"), "col")

    def local_factor(a_loc):
        n = a_loc.shape[0]
        W = 2 * NB
        dma = pltpu.SemaphoreType.DMA
        return pl.pallas_call(
            functools.partial(kernel, n),
            out_shape=jax.ShapeDtypeStruct(a_loc.shape, F32),
            in_specs=[pl.BlockSpec(memory_space=pl.ANY)],
            out_specs=pl.BlockSpec(memory_space=pl.ANY),
            scratch_shapes=[
                pltpu.VMEM((n * (n + 1) // 2 * W, W), F32),
                pltpu.VMEM((n * n // 4 * W, W), BF16),
                pltpu.VMEM((n * n // 4 * W, W), BF16),
                pltpu.VMEM((n * n // 4 * W, W), BF16),
                pltpu.VMEM((3, W, W), BF16),
                pltpu.VMEM((3, W, W), BF16),
                pltpu.VMEM((2, W, W), F32),
                pltpu.VMEM((NB, NB), F32),
                pltpu.VMEM((NB, NB), F32),
                pltpu.VMEM((2, NB, NB), F32),
                pltpu.VMEM((NB, NB), F32),
                dma((n, n // 2)), dma((n, n // 2)), dma((n, n // 2)), dma((4, n // 2)), dma((n, n // 2)), dma((n,)), dma((n,)),
                dma((2,)), dma, dma, dma((n // 2,)), dma, dma,
            ],
            compiler_params=pltpu.CompilerParams(
                vmem_limit_bytes=60 << 20, collective_id=0, has_side_effects=True),
        )(a_loc)

    return jax.shard_map(local_factor, mesh=mesh, in_specs=grid_spec, out_specs=grid_spec, check_vma=False)
```
